32 devices in a mesh: section: 2 (over x), lat: 4 (over z), lon: 4 (over y, core).
Axes of the slice: x: 2, y: 2, z: 4, core: 2. Of those that a mesh axis runs over, the one named last changes fastest.
Arguments:
- state: bfloat16 [2, 112, 360, 1024], P('section', 'lat', 'lon'), may hold values from -6 to 6
- fresh: bfloat16 [112, 360, 1024], P('lat', 'lon'), may hold values from -6 to 6
- cutoff: int32 [3], replicated, may hold values from 0 to 15
- plan: int32 [2, 2], replicated, may hold values from 0 to 1
- lmax: int32 [2], replicated, may hold values from 56 to 112, as said below
- mmax: int32 [2], replicated, may hold values from 24 to 96, as said below
- cutoff_table: float32 [16, 1024], replicated, may hold values from -3 to 3
- norm_gains: float32 [2, 2, 2, 1024], P('section'), may hold values from 0.1 to 1.9
- filters: float32 [2, 2, 2, 112, 1024], P('section', None, None, None, 'lon'), may hold values from -5 to 5
- w_in: bfloat16 [2, 2, 1024, 4096], P('section', None, 'lat'), may hold values from -0.1875 to 0.1875
- w_out: bfloat16 [2, 2, 1024, 4096], P('section', None, 'lat'), may hold values from -0.09375 to 0.09375
Outputs:
- first_pass: bfloat16 [2, 112, 360, 1024], P('section', 'lat', 'lon')
- second_pass: bfloat16 [2, 112, 360, 1024], P('section', 'lat', 'lon')
The draws below stay inside these ranges and needn't reach their ends.
Inputs may be any that keep to these rules, and one draw needn't show every extreme that they name: `lmax`: some section keeps all 112 degrees in every draw. `mmax`: some section keeps all 96 wavenumbers in every draw.
All inputs are finite; a program needn't handle non-finite values.
Results may differ from the reference program's by a relative error of at most 0.01.
Values may be sent and summed in bfloat16 or wider, within the bound.
No kernel may reach another device: no remote copies, remote signals or barrier semaphores. Data moves between devices by JAX's collectives and lax.ppermute only.
A program may use at most 384 MiB of HBM per device.

```python
import math
import jax
import jax.numpy as jnp
from jax import lax

D = 1024
FF = 4096
NLAT = 112
NLON = 360
MM = 96
LL = 112
NB = 2
NCUT = 16
SECTIONS = 2


def draw_bounded(key, lowest, highest):
    values = jax.random.randint(jax.random.fold_in(key, 11), (SECTIONS,), lowest, highest + 1)
    where_top = jax.random.randint(jax.random.fold_in(key, 23), (), 0, SECTIONS)
    return jnp.where(jnp.arange(SECTIONS) == where_top, highest, values).astype(jnp.int32)


def draw_lmax(key, part):
    return draw_bounded(jax.random.fold_in(key, 101), LL // 2, LL)


def draw_mmax(key, part):
    return draw_bounded(jax.random.fold_in(key, 202), MM // 4, MM)


def touch_ends(result, own_key, low, top_value):
    longest = result.shape.index(max(result.shape))
    spots = []
    for shift in (0, 1):
        where = [jax.random.randint(jax.random.fold_in(own_key, axis), (), 0, length) for axis, length in enumerate(result.shape)]
        where[longest] = (where[longest] + shift) % result.shape[longest]
        spots.append(tuple(where))
    return result.at[spots[0]].set(low).at[spots[1]].set(top_value)


def steps_of(stream_key, extent, shards, least, top_value):
    def one(position, blocks):
        heights = jax.random.uniform(jax.random.fold_in(jax.random.fold_in(stream_key, 6), position), (blocks,), jnp.float32, least / len(shards), top_value / len(shards))
        return jnp.repeat(jnp.exp(heights), extent[position] // blocks).reshape((-1,) + (1,) * (len(extent) - position - 1))

    loudness = one(*shards[0])
    for cut in shards[1:]:
        loudness = loudness * one(*cut)
    return loudness


def normal_values(stream_key, extent, deviation, reach, split=(), kind=jnp.bfloat16):
    entries = deviation * jax.random.normal(stream_key, extent, jnp.float32)
    if split:
        entries = entries * steps_of(stream_key, extent, split, -0.22, 0.18)
    return jnp.clip(entries, -reach, reach).astype(kind)


def setup_inputs(seed: int = 0) -> dict:
    arg_keys = jax.random.split(jax.random.key(seed), 12)
    state = normal_values(arg_keys[0], (SECTIONS, NLAT, NLON, D), 1.0, 6.0, ((0, 2), (1, 4), (2, 4)))
    fresh = normal_values(arg_keys[1], (NLAT, NLON, D), 1.0, 6.0, ((0, 4), (1, 4)))
    cutoff = jax.random.randint(arg_keys[2], (SECTIONS + 1,), 0, NCUT).astype(jnp.int32)
    plan = touch_ends(jax.random.randint(arg_keys[3], (2, SECTIONS), 0, NB), jax.random.fold_in(arg_keys[3], 1), 0, NB - 1).astype(jnp.int32)
    lmax = draw_lmax(jax.random.fold_in(arg_keys[11], 71), 0)
    mmax = draw_mmax(jax.random.fold_in(arg_keys[11], 71), 0)
    cutoff_table = normal_values(arg_keys[6], (NCUT, D), 0.5, 3.0, (), jnp.float32)
    norm_gains = jnp.clip(1.0 + 0.18 * jax.random.normal(arg_keys[7], (SECTIONS, NB, 2, D), jnp.float32), 0.1, 1.9)
    filters = normal_values(arg_keys[8], (SECTIONS, NB, 2, LL, D), 1.0, 5.0, ((0, 2), (4, 4)), jnp.float32)
    w_in = normal_values(arg_keys[9], (SECTIONS, NB, D, FF), D ** -0.5, 0.1875, ((0, 2), (2, 4)))
    w_out = normal_values(arg_keys[10], (SECTIONS, NB, D, FF), FF ** -0.5, 0.09375, ((0, 2), (2, 4)))
    return {"state": state, "fresh": fresh, "cutoff": cutoff, "plan": plan, "lmax": lmax, "mmax": mmax, "cutoff_table": cutoff_table, "norm_gains": norm_gains, "filters": filters, "w_in": w_in, "w_out": w_out}


def legendre_table(orders):
    rows = jnp.arange(NLAT, dtype=jnp.float32)
    theta = math.pi * (rows + 0.5) / NLAT
    cosine = jnp.cos(theta)
    sine = jnp.sin(theta)
    order = orders[:, None]
    log_start = 0.5 * jnp.log((2.0 * order + 1.0) / (4.0 * math.pi)) + jax.scipy.special.gammaln(order + 0.5) - jax.scipy.special.gammaln(0.5) - jax.scipy.special.gammaln(order + 1.0) + order * jnp.log(sine)[None, :]
    start = jnp.exp(log_start)

    def advance(carry, degree):
        last, before = carry
        level = degree.astype(jnp.float32)
        coef_a = jnp.sqrt(jnp.maximum(4.0 * level * level - 1.0, 1.0) / jnp.maximum(level * level - order * order, 1.0))
        coef_b = jnp.sqrt(jnp.maximum((level - 1.0) ** 2 - order * order, 0.0) / jnp.maximum(4.0 * (level - 1.0) ** 2 - 1.0, 1.0))
        general = coef_a * (cosine[None, :] * last - coef_b * before)
        fresh_row = jnp.where(level < order, jnp.zeros_like(start), jnp.where(level == order, start, general))
        return ((fresh_row, last), fresh_row)
    _, table = lax.scan(advance, (jnp.zeros_like(start), jnp.zeros_like(start)), jnp.arange(LL, dtype=jnp.int32))
    return table

def quadrature():
    rows = jnp.arange(NLAT, dtype=jnp.float32)
    theta = math.pi * (rows + 0.5) / NLAT
    return 2.0 * math.pi * (math.pi / NLAT) * jnp.sin(theta)

def fourier_tables(n_lon):
    columns = jnp.arange(n_lon, dtype=jnp.int32)
    orders = jnp.arange(MM, dtype=jnp.int32)
    phase = 2.0 * math.pi * (columns[:, None] * orders[None, :] % n_lon).astype(jnp.float32) / n_lon
    cos_fwd = jnp.cos(phase) / n_lon
    sin_fwd = -jnp.sin(phase) / n_lon
    weight = jnp.where(orders == 0, 1.0, 2.0).astype(jnp.float32)[:, None]
    inverse = jnp.stack([weight * jnp.cos(phase).T, -weight * jnp.sin(phase).T], 0)
    return (cos_fwd, sin_fwd, inverse)

def layer_norm(values, gain):
    center = values - lax.optimization_barrier(jnp.mean(values, axis=-1, keepdims=True))
    spread = lax.optimization_barrier(jnp.mean(center * center, axis=-1, keepdims=True))
    return center * lax.rsqrt(spread + 1e-05) * gain

def run_block(tokens, cut, gains, filt, weight_in, weight_out, l_max, m_max, cutoff_table, tables):
    plain, weighted, cos_fwd, sin_fwd, inverse = tables
    highest = lax.Precision.HIGHEST
    onehot = (jnp.arange(NCUT, dtype=jnp.int32) == cut).astype(jnp.float32)
    embed = jnp.dot(onehot, cutoff_table, precision=highest)
    base = tokens.astype(jnp.float32) + embed
    normed = layer_norm(base, gains[0]).astype(jnp.bfloat16)
    wide = normed.astype(jnp.float32)
    real_part = jnp.einsum('jkc,km->jmc', wide, cos_fwd, precision=highest)
    imag_part = jnp.einsum('jkc,km->jmc', wide, sin_fwd, precision=highest)
    spectrum = jnp.stack([real_part, imag_part], 1).astype(jnp.bfloat16)
    coeff = jnp.einsum('lmj,jrmc->rlmc', weighted, spectrum.astype(jnp.float32), precision=highest)
    keep = ((jnp.arange(LL, dtype=jnp.int32) < l_max)[:, None] & (jnp.arange(MM, dtype=jnp.int32) < m_max)[None, :]).astype(jnp.float32)[:, :, None]
    filt_re = filt[0][:, None, :]
    filt_im = filt[1][:, None, :]
    out_re = keep * (coeff[0] * filt_re - coeff[1] * filt_im)
    out_im = keep * (coeff[0] * filt_im + coeff[1] * filt_re)
    synthesis = jnp.einsum('lmj,rlmc->jrmc', plain, jnp.stack([out_re, out_im], 0), precision=highest).astype(jnp.bfloat16)
    spectral = jnp.einsum('jrmc,rmk->jkc', synthesis.astype(jnp.float32), inverse, precision=highest).astype(jnp.bfloat16)
    mixed = base + spectral.astype(jnp.float32)
    normed_two = layer_norm(mixed, gains[1]).astype(jnp.bfloat16)
    flat = normed_two.reshape(-1, normed_two.shape[-1])
    hidden = jax.nn.gelu(jnp.dot(flat, weight_in, preferred_element_type=jnp.float32)).astype(jnp.bfloat16)
    projected = lax.dot_general(hidden, weight_out, (((1,), (1,)), ((), ())), preferred_element_type=jnp.float32)
    return (mixed + projected.reshape(mixed.shape)).astype(jnp.bfloat16)

def reference(state, fresh, cutoff, plan, lmax, mmax, cutoff_table, norm_gains, filters, w_in, w_out):
    plain = legendre_table(jnp.arange(MM, dtype=jnp.float32))
    weighted = plain * quadrature()[None, None, :]
    cos_fwd, sin_fwd, inverse = fourier_tables(NLON)
    tables = (plain, weighted, cos_fwd, sin_fwd, inverse)

    def apply(tokens, section_num, tick):
        block_num = plan[tick, section_num]
        cut = cutoff[tick - section_num + SECTIONS - 1]
        gains = lax.dynamic_index_in_dim(norm_gains[section_num], block_num, 0, keepdims=False)
        filt = lax.dynamic_index_in_dim(filters[section_num], block_num, 0, keepdims=False)
        weight_in = lax.dynamic_index_in_dim(w_in[section_num], block_num, 0, keepdims=False)
        weight_out = lax.dynamic_index_in_dim(w_out[section_num], block_num, 0, keepdims=False)
        return run_block(tokens, cut, gains, filt, weight_in, weight_out, lmax[section_num], mmax[section_num], cutoff_table, tables)
    first = [apply(state[section_num], section_num, 0) for section_num in range(SECTIONS)]
    second = []
    for section_num in range(SECTIONS):
        incoming = fresh if section_num == 0 else first[section_num - 1]
        second.append(apply(incoming, section_num, 1))
    return (jnp.stack(first, 0), jnp.stack(second, 0))
```

```python
import functools
import math

import jax
import jax.numpy as jnp
from jax import lax
from jax.experimental import pallas as pl
from jax.experimental.pallas import tpu as pltpu
from jax.sharding import PartitionSpec as P


MM = 96
CHUNKS = 4

F32 = jnp.float32
BF16 = jnp.bfloat16
VMEM = 56 * 1024 * 1024


def chunks_of(n_rows):
    return CHUNKS if n_rows % CHUNKS == 0 else 1


def round_up(value, step):
    return (value + step - 1) // step * step


def exchange(values, axis):
    count = lax.axis_size(axis)
    got = [values[0]]
    for offset in range(1, count):
        pairs = [(s, (s + offset) % count) for s in range(count)]
        got.append(lax.ppermute(values[offset], axis, pairs))
    return got


def cost(flops, nbytes, trans=0):
    return pl.CostEstimate(flops=int(flops), bytes_accessed=int(nbytes), transcendentals=int(trans))


class Order:
    def __init__(self):
        self.last = []

    def call(self, kernel, operands, in_specs, **kwargs):
        deps = [d for d in self.last if all(d is not o for o in operands)]
        n_dep = len(deps)
        n_in = len(operands)

        def body(*refs):
            kernel(*refs[:n_in], *refs[n_in + n_dep :])

        outs = pl.pallas_call(
            body,
            in_specs=in_specs + [pl.BlockSpec(memory_space=pl.ANY)] * n_dep,
            compiler_params=params(),
            **kwargs,
        )(*operands, *deps)
        self.last = [outs[0]]
        return outs


def params(n_grid=1):
    return pltpu.CompilerParams(vmem_limit_bytes=VMEM, dimension_semantics=("arbitrary",) * n_grid)


def legendre_kernel(order_ref, cos_ref, start_ref, zero_ref, out_ref):
    order = order_ref[...]
    cosine = cos_ref[...]
    start = start_ref[...]
    zero = zero_ref[...]

    def advance(degree, carry):
        last, before = carry
        level = degree.astype(F32)
        coef_a = jnp.sqrt(
            jnp.maximum(4.0 * level * level - 1.0, 1.0)
            / jnp.maximum(level * level - order * order, 1.0)
        )
        coef_b = jnp.sqrt(
            jnp.maximum((level - 1.0) ** 2 - order * order, 0.0)
            / jnp.maximum(4.0 * (level - 1.0) ** 2 - 1.0, 1.0)
        )
        general = coef_a * (cosine * last - coef_b * before)
        row = jnp.where(level < order, zero, jnp.where(level == order, start, general))
        out_ref[degree] = row
        return (row, last)

    lax.fori_loop(0, out_ref.shape[0], advance, (zero, zero))


def legendre_table(orders, rows, n_rows, n_degrees):
    theta = math.pi * (rows.astype(F32) + 0.5) / n_rows
    cosine = jnp.cos(theta)
    sine = jnp.sin(theta)
    order = orders.astype(F32)[:, None]
    log_start = (
        0.5 * jnp.log((2.0 * order + 1.0) / (4.0 * math.pi))
        + jax.scipy.special.gammaln(order + 0.5)
        - jax.scipy.special.gammaln(0.5)
        - jax.scipy.special.gammaln(order + 1.0)
        + order * jnp.log(sine)[None, :]
    )
    start = jnp.exp(log_start)
    table = pl.pallas_call(
        legendre_kernel,
        out_shape=jax.ShapeDtypeStruct((n_degrees,) + start.shape, F32),
        name="legendre",
        cost_estimate=cost(1e6, 4 * n_degrees * start.size),
    )(jnp.broadcast_to(order, start.shape), jnp.broadcast_to(cosine[None, :], start.shape), start, jnp.zeros_like(start))
    quad = 2.0 * math.pi * (math.pi / n_rows) * sine
    return table, quad


def fourier_tables(n_lon):
    columns = jnp.arange(n_lon, dtype=jnp.int32)
    orders = jnp.arange(MM, dtype=jnp.int32)
    phase = 2.0 * math.pi * (columns[:, None] * orders[None, :] % n_lon).astype(F32) / n_lon
    weight = jnp.where(orders == 0, 1.0, 2.0).astype(F32)[None, :]
    forward = jnp.stack([jnp.cos(phase), -jnp.sin(phase)], 0) / n_lon
    inverse = jnp.stack([weight * jnp.cos(phase), -weight * jnp.sin(phase)], 0)
    return forward, inverse


def pick_tokens(flag_ref, tok_refs, row):
    if len(tok_refs) == 1:
        return tok_refs[0][row].astype(F32)
    return jnp.where(flag_ref[0] == 0, tok_refs[0][row].astype(F32), tok_refs[1][row].astype(F32))


def norm_rows(values, gain):
    center = values - jnp.mean(values, axis=-1, keepdims=True)
    spread = jnp.mean(center * center, axis=-1, keepdims=True)
    return center * lax.rsqrt(spread + 1e-05) * gain


def norm_kernel(n_tok, flag_ref, off_ref, *refs):
    tok_refs = refs[:n_tok]
    emb_ref, gain_ref = refs[n_tok : n_tok + 2]
    outs = refs[n_tok + 2 : -1]
    scr = refs[-1]
    cols = tok_refs[0].shape[1]
    part = outs[0].shape[-1]
    scr[...] = jnp.zeros_like(scr)

    def one(row, carry):
        x = pick_tokens(flag_ref, tok_refs, row) + emb_ref[...]
        scr[pl.ds(0, cols), :] = norm_rows(x, gain_ref[...]).astype(BF16)
        for o, out in enumerate(outs):
            out[row] = scr[:, pl.ds(pl.multiple_of(off_ref[o], 128), part)]
        return carry

    lax.fori_loop(0, tok_refs[0].shape[0], one, 0)


def dft_kernel(n_in, *refs):
    table_ref = refs[0]
    ins = refs[1 : 1 + n_in]
    outs = refs[1 + n_in :]
    height = outs[0].shape[1]

    def one(row, carry):
        wide = jnp.concatenate([r[row] for r in ins], axis=0)
        res = jnp.dot(table_ref[...], wide, preferred_element_type=F32).astype(BF16)
        for o, out in enumerate(outs):
            out[row] = res[o * height : (o + 1) * height]
        return carry

    lax.fori_loop(0, ins[0].shape[0], one, 0)


def spectral_kernel(n_in, m_local, *refs):
    ana_ref, syn_ref, filt_ref = refs[:3]
    ins = refs[3 : 3 + n_in]
    outs = refs[3 + n_in : 3 + 2 * n_in]
    scr = refs[-1]
    rows, height, width = ins[0].shape
    total = rows * n_in
    for p, ref in enumerate(ins):
        scr[pl.ds(p * rows * height, rows * height), :] = (
            ref[...].reshape(rows * height, width).astype(F32)
        )
    filt_re = filt_ref[0]
    filt_im = filt_ref[1]
    for m in range(m_local):
        at_re = pl.ds(m, total, stride=height)
        at_im = pl.ds(m_local + m, total, stride=height)
        both = jnp.concatenate([scr[at_re, :], scr[at_im, :]], axis=1).astype(BF16)
        coeff = jnp.dot(ana_ref[m], both, preferred_element_type=F32)
        c_re = coeff[:, :width]
        c_im = coeff[:, width:]
        out_re = c_re * filt_re - c_im * filt_im
        out_im = c_re * filt_im + c_im * filt_re
        filtered = jnp.concatenate([out_re, out_im], axis=1).astype(BF16)
        made = jnp.dot(syn_ref[m], filtered, preferred_element_type=F32)
        scr[at_re, :] = made[:, :width]
        scr[at_im, :] = made[:, width:]
    for p, ref in enumerate(outs):
        ref[...] = (
            scr[pl.ds(p * rows * height, rows * height), :].astype(BF16).reshape(rows, height, width)
        )


def gelu(x):
    inner = x * (0.7978845608028654 + 0.035677408136300125 * (x * x))
    half = 0.5 * x
    return half + half * jnp.tanh(inner)


def mlp_kernel(n_group, n_tok, n_lon, n_out, aliased, flag_ref, off_ref, *refs):
    n_all = n_group * n_tok
    tok_refs = [refs[g * n_tok : (g + 1) * n_tok] for g in range(n_group)]
    spec_refs = [refs[n_all + g * n_lon : n_all + (g + 1) * n_lon] for g in range(n_group)]
    base = n_all + n_group * n_lon
    emb_ref, gain_ref, win_ref, wout_ref = refs[base : base + 4]
    base += 5 if aliased else 4
    outs = refs[base : base + n_out]
    acc, n2, spec = refs[base + n_out :]
    rows, cols, width = tok_refs[0][0].shape
    part = spec_refs[0][0].shape[-1]
    height = acc.shape[0]
    block_f = win_ref.shape[-1]
    step = pl.program_id(0)

    @pl.when(step == 0)
    def _():
        used = n_group * rows * cols
        if height > used:
            tail = used // 8 * 8
            acc[pl.ds(tail, height - tail), :] = jnp.zeros((height - tail, width), F32)
        for g in range(n_group):
            for row in range(rows):
                for o, ref in enumerate(spec_refs[g]):
                    spec[:, pl.ds(pl.multiple_of(off_ref[o], 128), part)] = ref[row]
                u = pick_tokens(flag_ref, tok_refs[g], row) + emb_ref[...]
                at = pl.ds((g * rows + row) * cols, cols)
                acc[at, :] = u + spec[pl.ds(0, cols), :].astype(F32)

        def norm_block(i, carry):
            at = pl.ds(pl.multiple_of(i * 128, 128), 128)
            n2[at, :] = norm_rows(acc[at, :], gain_ref[...]).astype(BF16)
            return carry

        lax.fori_loop(0, height // 128, norm_block, 0)

    tile = 640 if height % 640 == 0 else 128
    for i in range(height // tile):
        at = pl.ds(i * tile, tile)
        weight_in = win_ref[...].reshape(width, block_f)
        weight_out = wout_ref[...].reshape(width, block_f)
        pre = jnp.dot(n2[at, :], weight_in, preferred_element_type=F32)
        hidden = gelu(pre).astype(BF16)
        acc[at, :] += lax.dot_general(
            hidden, weight_out, (((1,), (1,)), ((), ())), preferred_element_type=F32
        )

    @pl.when(step == pl.num_programs(0) - 1)
    def _():
        for row in range(n_group * rows):
            value = acc[pl.ds(row * cols, cols), :].astype(BF16)
            for out in outs:
                if len(out.shape) == 3:
                    out[row] = value
                else:
                    out[0, row] = value


def local(state, fresh, cutoff, plan, lmax, mmax, cutoff_table, norm_gains, filters, w_in, w_out):
    section_idx = lax.axis_index("section")
    lat_idx = lax.axis_index("lat")
    lon_idx = lax.axis_index("lon")
    n_section = lax.axis_size("section")
    n_lat = lax.axis_size("lat")
    n_lon = lax.axis_size("lon")
    n_rows, n_cols, width = fresh.shape
    n_degrees = filters.shape[3]
    ff = w_in.shape[3]
    part = width // n_lon
    all_rows = n_rows * n_lat
    all_cols = n_cols * n_lon
    m_local = MM // n_lat
    height = round_up(2 * m_local, 16)
    cols_pad = round_up(n_cols, 16)
    n_chunk = chunks_of(n_rows)
    rows = n_rows // n_chunk

    lon_fwd = (lon_idx + jnp.arange(n_lon, dtype=jnp.int32)) % n_lon
    lon_bwd = (lon_idx - jnp.arange(n_lon, dtype=jnp.int32)) % n_lon
    lat_fwd = (lat_idx + jnp.arange(n_lat, dtype=jnp.int32)) % n_lat
    lat_bwd = (lat_idx - jnp.arange(n_lat, dtype=jnp.int32)) % n_lat
    off_fwd = lon_fwd * part
    off_bwd = lon_bwd * part

    def gathered(tick):
        block = plan[tick, section_idx]
        local_rows = w_in.shape[2]
        piece = ff // n_lon
        start = (0, block, 0, lon_idx * piece)
        size = (1, 1, local_rows, piece)
        mine = jnp.concatenate(
            [lax.dynamic_slice(w_in, start, size)[0], lax.dynamic_slice(w_out, start, size)[0]], 0
        )
        rows_here = lax.all_gather(mine, "lat")
        return lax.all_gather(rows_here, "lon")

    weights = [gathered(t) for t in range(2)]

    forward, inverse = fourier_tables(all_cols)

    def modes(table, order):
        t = table.transpose(2, 0, 1).reshape(n_lat, m_local, 2, all_cols).transpose(0, 2, 1, 3)
        t = t.reshape(n_lat, 2 * m_local, all_cols)[order]
        return jnp.pad(t, ((0, 0), (0, height - 2 * m_local), (0, 0)))

    def columns(table, order):
        t = table.reshape(n_lat, height, n_lon, n_cols)[:, :, order]
        t = jnp.pad(t, ((0, 0), (0, 0), (0, 0), (0, cols_pad - n_cols)))
        return t.reshape(n_lat * height, n_lon * cols_pad)

    dft = columns(modes(forward, lat_fwd), lon_bwd).astype(BF16)
    idft = columns(modes(inverse, lat_bwd), lon_fwd).T.astype(BF16)

    orders = lat_idx * m_local + jnp.arange(m_local, dtype=jnp.int32)
    row_ids = (lat_bwd[:, None] * n_rows + jnp.arange(n_rows, dtype=jnp.int32)[None, :]).reshape(-1)
    table, quad = legendre_table(orders, row_ids, all_rows, n_degrees)
    m_max = mmax[section_idx]
    l_max = lmax[section_idx]
    ana = (table * quad[None, None, :]).astype(BF16).transpose(1, 0, 2)
    keep_m = (orders < m_max).astype(F32)
    syn = (table * keep_m[None, :, None]).astype(BF16).transpose(1, 2, 0)
    back = [(n_lat - o) % n_lat for o in range(n_lat)]
    syn = syn.reshape(m_local, n_lat, n_rows, n_degrees)
    syn = jnp.concatenate([syn[:, b : b + 1] for b in back], 1).reshape(m_local, all_rows, n_degrees)
    keep_l = (jnp.arange(n_degrees, dtype=jnp.int32) < l_max)[None, :, None]

    smem = pl.BlockSpec(memory_space=pltpu.SMEM)
    whole = pl.BlockSpec(memory_space=pltpu.VMEM)
    flag = section_idx.astype(jnp.int32).reshape(1)
    token_block = (rows, n_cols, width)

    def token_specs(tokens, chunk):
        specs = []
        for t in tokens:
            if t.shape[0] == rows and n_chunk > 1:
                specs.append(pl.BlockSpec(token_block, lambda *_: (0, 0, 0)))
            else:
                specs.append(pl.BlockSpec(token_block, lambda *_, c=chunk: (c, 0, 0)))
        return specs

    order = Order()

    def norm_call(tokens, chunk, emb, gain):
        piece = jax.ShapeDtypeStruct((rows, cols_pad, part), BF16)
        return order.call(
            functools.partial(norm_kernel, len(tokens)),
            [flag, off_fwd, *tokens, emb, gain],
            [smem, smem] + token_specs(tokens, chunk) + [whole, whole],
            grid=(1,),
            out_specs=[pl.BlockSpec((rows, cols_pad, part), lambda i: (0, 0, 0))] * n_lon,
            out_shape=[piece] * n_lon,
            scratch_shapes=[pltpu.VMEM((cols_pad, width), BF16)],
            name="norm",
            cost_estimate=cost(4e9 / n_chunk, 4 * rows * n_cols * width),
        )

    def table_call(table, pieces, n_out, out_height, name):
        r, h, c = pieces[0].shape
        return order.call(
            functools.partial(dft_kernel, len(pieces)),
            [table, *pieces],
            [whole] * (1 + len(pieces)),
            grid=(1,),
            out_specs=[whole] * n_out,
            out_shape=[jax.ShapeDtypeStruct((r, out_height, c), BF16)] * n_out,
            name=name,
            cost_estimate=cost(4 * table.size * c * r, 4 * r * h * c * len(pieces)),
        )

    def spectral_call(pieces, filt):
        n_in = len(pieces)
        half = 128 if part % 128 == 0 else part
        tables = pl.BlockSpec(memory_space=pltpu.VMEM)
        block = pl.BlockSpec((rows, height, half), lambda i: (0, 0, i))
        return order.call(
            functools.partial(spectral_kernel, n_in, m_local),
            [ana, syn, filt, *pieces],
            [tables, tables, pl.BlockSpec((2, n_degrees, half), lambda i: (0, 0, i))]
            + [block] * n_in,
            grid=(part // half,),
            out_specs=[block] * n_in,
            out_shape=[jax.ShapeDtypeStruct((rows, height, part), BF16)] * n_in,
            scratch_shapes=[pltpu.VMEM((all_rows * height, half), F32)],
            name="spectral",
            cost_estimate=cost(8e9, 8e6),
        )

    def mlp_call(chunks, tokens, spec, emb, gain, weight, full, want_chunk):
        n_group = len(chunks)
        block_f = min(512, ff // n_lon)
        per = ff // n_lon // block_f
        m_pad = round_up(n_group * rows * n_cols, 128)
        n_tok = len(tokens[0])
        chunk_shape = jax.ShapeDtypeStruct(token_block, BF16)
        full_shape = jax.ShapeDtypeStruct((1, n_rows, n_cols, width), BF16)
        out_shape = [full_shape] + ([chunk_shape] if want_chunk else [])
        at = chunks[0] // n_group
        out_specs = [
            pl.BlockSpec((1, n_group * rows, n_cols, width), lambda i, at=at: (0, at, 0, 0))
        ]
        if want_chunk:
            out_specs.append(pl.BlockSpec(token_block, lambda i: (0, 0, 0)))
        block = (None, n_lat, None, weight.shape[3], block_f)
        in_specs = [smem, smem]
        for c, t in zip(chunks, tokens):
            in_specs += token_specs(t, c)
        in_specs += [whole] * (n_group * n_lon + 2)
        in_specs += [
            pl.BlockSpec(block, lambda i: (i // per, 0, 0, 0, i % per)),
            pl.BlockSpec(block, lambda i: (i // per, 0, 1, 0, i % per)),
        ]
        args = [flag, off_bwd]
        for t in tokens:
            args += t
        for s in spec:
            args += s
        args += [emb, gain, weight, weight]
        aliases = {}
        if full is not None:
            in_specs.append(pl.BlockSpec(memory_space=pl.ANY))
            aliases = {len(args): 0}
            args.append(full)
        return order.call(
            functools.partial(mlp_kernel, n_group, n_tok, n_lon, len(out_shape), full is not None),
            args,
            in_specs,
            grid=(ff // block_f,),
            out_specs=out_specs,
            out_shape=out_shape,
            scratch_shapes=[
                pltpu.VMEM((m_pad, width), F32),
                pltpu.VMEM((m_pad, width), BF16),
                pltpu.VMEM((cols_pad, width), BF16),
            ],
            input_output_aliases=aliases,
            name="mlp",
            cost_estimate=cost(4 * m_pad * width * ff, 4 * width * ff, m_pad * ff),
        )

    def settings(tick):
        block = plan[tick, section_idx]
        cut = cutoff[tick - section_idx + n_section - 1]
        gains = norm_gains[0, block]
        filt = jnp.where(keep_l, filters[0, block], 0.0)
        emb = cutoff_table[cut][None, :]
        return emb, gains[0:1], gains[1:2], filt

    pass_on = [(s, s + 1) for s in range(n_section - 1)]
    ticks = [settings(0), settings(1)]
    tokens = [[[state[0]]] * n_chunk, [None] * n_chunk]
    lonf, latf, latb, lonb = {}, {}, {}, {}
    full = [None, None]

    def do_norm(t, c):
        emb, gain_a, _, _ = ticks[t]
        sent = norm_call(tokens[t][c], c, emb, gain_a)
        lonf[t, c] = exchange(sent, "lon")

    def do_dft(t, c):
        made = table_call(dft, lonf[t, c], n_lat, height, "dft")
        latf[t, c] = exchange(made, "lat")

    def do_spectral(t):
        pieces = [latf[t, c][o] for o in range(n_lat) for c in range(n_chunk)]
        made = spectral_call(pieces, ticks[t][3])
        for c in range(n_chunk):
            latb[t, c] = exchange([made[o * n_chunk + c] for o in range(n_lat)], "lat")

    def do_idft(t, c):
        made = table_call(idft, latb[t, c], n_lon, cols_pad, "idft")
        lonb[t, c] = exchange(made, "lon")

    def do_mlp(t, c):
        emb, _, gain_b, _ = ticks[t]
        group = [c] if t == 0 or n_chunk % 2 else [c, c + 1]
        outs = mlp_call(
            group, [tokens[t][g] for g in group], [lonb[t, g] for g in group],
            emb, gain_b, weights[t], full[t], t == 0,
        )
        full[t] = outs[0]
        if t == 0:
            handed = lax.ppermute(outs[1], "section", pass_on)
            tokens[1][c] = [fresh, handed]

    steps = {"N": do_norm, "D": do_dft, "S": lambda t, c: do_spectral(t), "I": do_idft, "M": do_mlp}
    for kind, t, c in kernel_order(n_chunk):
        if (kind, t, c) == ("D", 0, n_chunk // 3):
            order.last = order.last + [ana, syn]
        steps[kind](t, c)
    return (full[0], full[1])


def kernel_order(n_chunk):
    if n_chunk == 4:
        text = (
            "N00 N01 N02 N03",
            "D00 D01 D02 D03",
            "S00 I00 I01 M00",
            "I02 M01 N10 I03",
            "M02 N11 D10 M03",
            "N12 D11 N13 D12",
            "D13 S10 I10 I11",
            "I12 I13 M10 M12",
        )
        return [(w[0], int(w[1]), int(w[2])) for w in " ".join(text).split()]
    every = range(n_chunk)
    order = []
    for t in range(2):
        order += [("N", t, c) for c in every] + [("D", t, c) for c in every] + [("S", t, 0)]
        order += [("I", t, c) for c in every] + [("M", t, c) for c in every]
    return order


def solution(mesh):
    return jax.shard_map(
        local,
        mesh=mesh,
        in_specs=(
            P("section", "lat", "lon", None),
            P("lat", "lon", None),
            P(),
            P(),
            P(),
            P(),
            P(),
            P("section", None, None, None),
            P("section", None, None, None, "lon"),
            P("section", None, "lat", None),
            P("section", None, "lat", None),
        ),
        out_specs=(P("section", "lat", "lon", None), P("section", "lat", "lon", None)),
        check_vma=False,
    )
```
